32 devices in a mesh: dp: 4 (over y, x), cls: 8 (over z, core).
Axes of the slice: x: 2, y: 2, z: 4, core: 2. Of those that a mesh axis runs over, the one named last changes fastest.
Arguments:
- sketches: bfloat16 [8192, 4096], P(('dp', 'cls')), may hold values from -6 to 6
- labels: int32 [8192], P(('dp', 'cls')), may hold values from 0 to 7, as said below
- places: int32 [8192], P(('dp', 'cls')), may hold values from 0 to 2047, as said below
- counts: int32 [8, 4, 32], P('cls'), may hold values from 0 to 16, as said below
- chosen: int32 [3, 8], P(None, 'cls'), may hold values from 0 to 2047, as said below
Outputs:
- gain_scores: float32 [3, 8, 2048], P(None, 'cls', 'dp')
- coverage: float32 [8, 2048], P('cls', 'dp')
The draws below stay inside these ranges and needn't reach their ends.
Inputs may be any that keep to these rules, and one draw needn't show every extreme that they name: `labels`: every class has 4 or more examples. `places`: an example of device s (its index along dp and cls together) with class k has place m * 512 + s * 16 + j in class k's block: m is the member of dp that receives it, and for each k, m and s the j run over 0 to counts[k, m, s] - 1 without gaps, so no two examples share a place. In every draw one class and member receive 16 examples from every device. counts[k, m, s] is the number of examples of device s that take places of class k on member m. chosen[t, k] is a place of class k's block that holds an example; the 3 picks of a class differ.
All inputs are finite; a program needn't handle non-finite values.
Results may differ from the reference program's by a relative error of at most 0.0003.
Values may be sent and summed in bfloat16 or wider, within the bound.
A program may use at most 128 MiB of HBM per device.

```python
import jax
import jax.numpy as jnp
from jax import lax

D = 4096
ROW_DEV = 256
STEPS = 3
CLASSES = 8
SUB = 16
CAP = 512
BLOCK = 2048
ROWS = 8192
N_DP = 4
DEVICES = 32


def layout_tables(key):
    slot_count = 2 * ROW_DEV
    class_key, full_key, member_key, base_key, pick_key = jax.random.split(jax.random.fold_in(key, 7), 5)
    class_level = jax.random.randint(class_key, (CLASSES,), 0, 3)
    full_class = jax.random.randint(full_key, (), 0, CLASSES)
    full_member = jax.random.randint(member_key, (), 0, N_DP)
    item_index = jnp.arange(slot_count, dtype=jnp.int32)
    item_member = item_index // (CLASSES * SUB)
    item_class = item_index // SUB % CLASSES
    item_place = item_index % SUB
    source = jnp.arange(DEVICES, dtype=jnp.int32)[:, None]
    promised = (item_class[None, :] == source % CLASSES) & (item_member[None, :] == source // CLASSES % N_DP) & (item_place[None, :] == 0)
    full_item = (item_class == full_class) & (item_member == full_member)
    base = jax.random.randint(base_key, (DEVICES, slot_count), 0, 2 ** 16)
    level = base + class_level[item_class][None, :] * 2 ** 16 + promised.astype(jnp.int32) * 2 ** 18 + full_item.astype(jnp.int32)[None, :] * 2 ** 19
    score = level * slot_count + item_index[None, :]
    top_scores, picked_items = lax.top_k(score, ROW_DEV)
    group = picked_items // SUB
    same_group = group[:, :, None] == group[:, None, :]
    earlier = picked_items[:, None, :] < picked_items[:, :, None]
    rank = jnp.sum((same_group & earlier).astype(jnp.int32), axis=2)
    member = group // CLASSES
    klass = group % CLASSES
    places = member * CAP + source * SUB + rank
    group_hits = (group[:, :, None] == jnp.arange(N_DP * CLASSES, dtype=jnp.int32)[None, None, :]).astype(jnp.int32)
    per_group = jnp.sum(group_hits, axis=1).reshape(DEVICES, N_DP, CLASSES)
    counts = jnp.transpose(per_group, (2, 1, 0))
    valid = (jnp.arange(SUB, dtype=jnp.int32)[None, None, None, :] < counts[:, :, :, None]).reshape(CLASSES, BLOCK)
    noise = jax.random.randint(pick_key, (CLASSES, BLOCK), 0, 256)
    pick_score = (noise + valid.astype(jnp.int32) * 512) * BLOCK + jnp.arange(BLOCK, dtype=jnp.int32)[None, :]
    top_picks, pick_places = lax.top_k(pick_score, STEPS)
    return (klass.reshape(-1), places.reshape(-1), counts, jnp.transpose(pick_places))


def draw_labels(key, part):
    return layout_tables(key)[0].astype(jnp.int32)


def draw_places(key, part):
    return layout_tables(key)[1].astype(jnp.int32)


def draw_counts(key, part):
    return layout_tables(key)[2].astype(jnp.int32)


def draw_chosen(key, part):
    return layout_tables(key)[3].astype(jnp.int32)


def draw_sketches(key, part):
    labels = layout_tables(key)[0].astype(jnp.int32)
    mean_key, noise_key, scale_key = jax.random.split(jax.random.fold_in(key, 11), 3)
    class_means = jnp.clip(jax.random.normal(mean_key, (CLASSES, D), jnp.float32), -4.2, 4.2)
    centers = 0.6 * class_means[labels]
    noise = jnp.clip(jax.random.normal(noise_key, (ROWS, D), jnp.float32), -4.2, 4.2)
    raw = centers + noise
    row_rms = jnp.sqrt(jnp.mean(raw * raw, axis=1, keepdims=True))
    scale = jnp.exp(jax.random.uniform(scale_key, (ROWS, 1), jnp.float32, jnp.log(0.98), jnp.log(1.02)))
    values = jnp.clip(scale * raw / row_rms, -6.0, 6.0)
    return values.astype(jnp.bfloat16)


def setup_inputs(seed: int = 0) -> dict:
    seeds = jax.random.split(jax.random.key(seed), 6)
    sketches = draw_sketches(jax.random.fold_in(seeds[5], 71), 0)
    labels = draw_labels(jax.random.fold_in(seeds[5], 71), 0)
    places = draw_places(jax.random.fold_in(seeds[5], 71), 0)
    counts = draw_counts(jax.random.fold_in(seeds[5], 71), 0)
    chosen = draw_chosen(jax.random.fold_in(seeds[5], 71), 0)
    return {"sketches": sketches, "labels": labels, "places": places, "counts": counts, "chosen": chosen}


def class_scores(class_block, class_counts, class_picks):
    wide = class_block.astype(jnp.float32)
    norms = jnp.sum(wide * wide, axis=1)
    inner = jnp.dot(class_block, class_block.T, preferred_element_type=jnp.float32)
    spread = (norms[:, None] + norms[None, :] - 2.0 * inner) / D
    valid = (jnp.arange(SUB, dtype=jnp.int32)[None, None, :] < class_counts[:, :, None]).reshape(-1)
    weight = valid.astype(jnp.float32)
    bound = jnp.max(jnp.where(valid[:, None] & valid[None, :], spread, 0.0))
    similar = bound - spread
    total = jnp.sum(class_counts).astype(jnp.float32)
    cover = jnp.zeros((similar.shape[0],), jnp.float32)
    scores = []
    for turn_index in range(STEPS):
        scores.append(jnp.sum(weight[:, None] * jnp.maximum(similar - cover[:, None], 0.0), axis=0) * weight / total)
        column = lax.dynamic_index_in_dim(similar, class_picks[turn_index].astype(jnp.int32), 1, keepdims=False)
        cover = jnp.maximum(cover, column)
    return jnp.stack(scores), cover * weight


def score_item(packed):
    return class_scores(packed[0], packed[1], packed[2])


def reference(sketches, labels, places, counts, chosen):
    flat_index = (labels * BLOCK + places).astype(jnp.int32)
    blocks = jnp.zeros((CLASSES * BLOCK, D), sketches.dtype).at[flat_index].set(sketches)
    blocks = blocks.reshape(CLASSES, BLOCK, D)
    scores, cover = lax.map(score_item, (blocks, counts, jnp.transpose(chosen)))
    return jnp.transpose(scores, (1, 0, 2)), cover
```

```python
import functools

import jax
import jax.numpy as jnp
from jax import lax
from jax.experimental import pallas as pl
from jax.experimental.pallas import tpu as pltpu
from jax.sharding import PartitionSpec as P

MESH = pl.DeviceIdType.MESH


def ring_place(index):
    high = index // 2
    return 2 * high + (index % 2 + high) % 2


def ring_member(place):
    high = place // 2
    return 2 * high + (place % 2 + high) % 2


def exchange_kernel(members, owners, out_ref, rows_ref, a_send, a_recv, own_sem, b_send, b_recv):
    member = lax.axis_index("dp")
    owner = lax.axis_index("cls")
    half = members // 2
    place = ring_place(member)
    side = owner % 2
    step = 1 - 2 * side

    barrier = pltpu.get_barrier_semaphore()
    for hop in range(1, owners):
        pl.semaphore_signal(
            barrier, inc=1, device_id=(member, (owner + hop) % owners), device_id_type=MESH
        )
    for hop in range(1, members):
        pl.semaphore_signal(
            barrier,
            inc=1,
            device_id=(ring_member((place + hop) % members), owner),
            device_id_type=MESH,
        )
    pl.semaphore_wait(barrier, owners + members - 2)

    def dispatch(chunk, hop):
        target = (owner + hop) % owners
        return pltpu.make_async_remote_copy(
            src_ref=out_ref.at[target, chunk],
            dst_ref=rows_ref.at[0, chunk, owner],
            send_sem=a_send.at[chunk, hop - 1],
            recv_sem=a_recv.at[chunk, hop - 1],
            device_id=(member, target),
            device_id_type=MESH,
        )

    def own_copy(chunk):
        return pltpu.make_async_copy(
            out_ref.at[owner, chunk], rows_ref.at[0, chunk, owner], own_sem.at[chunk]
        )

    def share(chunk, hop):
        target = ring_member((place + step * hop + members) % members)
        return pltpu.make_async_remote_copy(
            src_ref=rows_ref.at[0, chunk],
            dst_ref=rows_ref.at[hop, chunk],
            send_sem=b_send.at[chunk, hop - 1],
            recv_sem=b_recv.at[chunk, hop - 1],
            device_id=(target, owner),
            device_id_type=MESH,
        )

    sends_half = (place // half + side) % 2 == 0
    gets_half = (place // half + side) % 2 == 1

    for chunk in range(members):
        own_copy(chunk).start()
        for hop in range(1, owners):
            dispatch(chunk, hop).start()
    for chunk in range(members):
        own_copy(chunk).wait()
        for hop in range(1, owners):
            dispatch(chunk, hop).wait_recv()

        @pl.when(sends_half)
        def _(chunk=chunk):
            share(chunk, half).start()

        for hop in range(1, half):
            share(chunk, hop).start()
    for chunk in range(members):
        for hop in range(1, owners):
            dispatch(chunk, hop).wait_send()
        for hop in range(1, half):
            share(chunk, hop).wait()

        @pl.when(sends_half)
        def _(chunk=chunk):
            share(chunk, half).wait_send()

        @pl.when(gets_half)
        def _(chunk=chunk):
            share(chunk, half).wait_recv()


def exchange(outgoing, members, owners):
    sub, width = outgoing.shape[2:]
    slots = members // 2 + 1
    return pl.pallas_call(
        functools.partial(exchange_kernel, members, owners),
        out_shape=jax.ShapeDtypeStruct((slots, members, owners, sub, width), outgoing.dtype),
        in_specs=[pl.BlockSpec(memory_space=pltpu.VMEM)],
        out_specs=pl.BlockSpec(memory_space=pltpu.VMEM),
        scratch_shapes=[
            pltpu.SemaphoreType.DMA((members, owners - 1)),
            pltpu.SemaphoreType.DMA((members, owners - 1)),
            pltpu.SemaphoreType.DMA((members,)),
            pltpu.SemaphoreType.DMA((members, members // 2)),
            pltpu.SemaphoreType.DMA((members, members // 2)),
        ],
        compiler_params=pltpu.CompilerParams(
            collective_id=0, has_side_effects=True, vmem_limit_bytes=60 * 1024 * 1024
        ),
    )(outgoing)


def body(sketches, labels, places, counts, chosen):
    row_count, width = sketches.shape
    members = lax.axis_size("dp")
    owners = lax.axis_size("cls")
    devices = members * owners
    sub = 2 * row_count // devices
    capacity = devices * sub
    half = members // 2
    slots = half + 1
    member = lax.axis_index("dp")
    owner = lax.axis_index("cls")
    picked = chosen[:, 0]
    pick_count = picked.shape[0]

    target = (labels * members + places // capacity) * sub + places % sub
    send_table = (
        lax.broadcasted_iota(jnp.int32, (2 * row_count, row_count), 0) == target[None, :]
    ).astype(jnp.bfloat16)
    outgoing = jnp.dot(send_table, sketches, preferred_element_type=jnp.float32).astype(
        jnp.bfloat16
    )
    rows = exchange(outgoing.reshape(owners, members, sub, width), members, owners)
    rows = rows.reshape(slots * capacity, width)
    own = rows[:capacity]

    step = 1 - 2 * (owner % 2)
    place = ring_place(member)
    slot_member = jnp.stack(
        [ring_member((place - step * hop + members) % members) for hop in range(slots)]
    )
    has_half = (place // half + owner % 2) % 2 == 1
    slot_here = (jnp.arange(slots) < half) | has_half

    class_counts = counts[0]
    valid_places = (
        lax.broadcasted_iota(jnp.int32, (members, devices, sub), 2) < class_counts[:, :, None]
    )
    valid_blocks = jnp.transpose(
        valid_places.reshape(members, members, owners, sub), (1, 0, 2, 3)
    ).reshape(members, capacity)
    slot_valid = (
        jnp.stack([lax.dynamic_index_in_dim(valid_blocks, slot_member[s], 0, False) for s in range(slots)])
        & slot_here[:, None]
    )
    column_valid = slot_valid.reshape(-1)
    own_valid = slot_valid[0]
    total = jnp.sum(class_counts).astype(jnp.float32)

    source = picked % capacity // sub
    pick_index = (picked // capacity * owners + source % owners) * sub + picked % sub
    pick_table = (
        (jnp.arange(capacity)[None, :] == pick_index[:, None])
        & (source // owners == member)[:, None]
    ).astype(jnp.bfloat16)
    pick_part = jnp.dot(pick_table, own, preferred_element_type=jnp.float32).astype(jnp.bfloat16)
    pick_rows = jnp.sum(
        lax.all_gather(pick_part, "dp", axis=0).astype(jnp.float32), axis=0
    ).astype(jnp.bfloat16)

    wide = rows.astype(jnp.float32)
    norms = jnp.sum(wide * wide, axis=1)
    wide_picks = pick_rows.astype(jnp.float32)
    pick_norms = jnp.sum(wide_picks * wide_picks, axis=1)
    contract = (((1,), (1,)), ((), ()))
    inner = lax.dot_general(own, rows, contract, preferred_element_type=jnp.float32)
    pick_inner = lax.dot_general(pick_rows, rows, contract, preferred_element_type=jnp.float32)
    spread = (norms[:capacity, None] + norms[None, :] - 2.0 * inner) / width
    pick_spread = (pick_norms[:, None] + norms[None, :] - 2.0 * pick_inner) / width

    largest = jnp.max(
        jnp.where(own_valid[:, None] & column_valid[None, :], spread, 0.0)
    )
    bound = jnp.max(lax.all_gather(largest.reshape(1), "dp", axis=0))

    pick_similar = bound - pick_spread
    current = jnp.zeros((slots * capacity,), jnp.float32)
    column_gain = []
    row_gain = []
    similar = bound - spread
    far = similar[:, capacity:]
    for turn in range(pick_count):
        near_cover = current[:capacity]
        column_gain.append(
            jnp.sum(
                jnp.where(
                    own_valid[:, None] & column_valid[None, :],
                    jnp.maximum(similar - near_cover[:, None], 0.0),
                    0.0,
                ),
                axis=0,
            )
        )
        row_gain.append(
            jnp.sum(
                jnp.where(
                    column_valid[None, capacity:],
                    jnp.maximum(far - current[None, capacity:], 0.0),
                    0.0,
                ),
                axis=1,
            )
        )
        current = jnp.maximum(current, pick_similar[turn])
    column_gain = jnp.stack(column_gain).reshape(pick_count, slots, capacity)
    near_gain = column_gain[:, 0] + jnp.stack(row_gain)
    own_cover = current[:capacity]

    near = jnp.concatenate([near_gain, own_cover[None]], axis=0)
    held = jnp.concatenate(
        [
            near[:, None],
            jnp.concatenate(
                [column_gain[:, 1:], jnp.zeros((1, slots - 1, capacity), jnp.float32)], axis=0
            ),
        ],
        axis=1,
    )
    spots = jnp.arange(members)[:, None] == slot_member[None, :]
    spots = spots & slot_here[None, :]
    placed = jnp.sum(jnp.where(spots[None, :, :, None], held[:, None], 0.0), axis=2)
    placed = placed.reshape(pick_count + 1, members, members, owners, sub)
    placed = jnp.transpose(placed, (2, 0, 1, 3, 4)).reshape(members, pick_count + 1, capacity)
    summed = jnp.sum(
        lax.all_to_all(placed, "dp", split_axis=0, concat_axis=0, tiled=True), axis=0
    )
    place_valid = lax.dynamic_index_in_dim(
        valid_places.reshape(members, capacity), member, 0, keepdims=False
    ).astype(jnp.float32)
    gain_scores = (summed[:pick_count] * place_valid[None, :] / total)[:, None, :]
    coverage = (summed[pick_count] * place_valid)[None, :]
    return (gain_scores, coverage)


def solution(mesh):
    placed = (
        P(("dp", "cls"), None),
        P(("dp", "cls")),
        P(("dp", "cls")),
        P("cls", None, None),
        P(None, "cls"),
    )
    return jax.shard_map(
        body,
        mesh=mesh,
        in_specs=placed,
        out_specs=(P(None, "cls", "dp"), P("cls", "dp")),
        check_vma=False,
    )
```

```python
import functools

import jax
import jax.numpy as jnp
from jax import lax
from jax.experimental import pallas as pl
from jax.experimental.pallas import tpu as pltpu
from jax.sharding import PartitionSpec as P

MESH = pl.DeviceIdType.MESH


def ring_place(index):
    high = index // 2
    return 2 * high + (index % 2 + high) % 2


def ring_member(place):
    high = place // 2
    return 2 * high + (place % 2 + high) % 2


def exchange_kernel(
    members,
    owners,
    out_ref,
    table_ref,
    inner_ref,
    pick_inner_ref,
    norms_ref,
    pick_norms_ref,
    rows_ref,
    picks_ref,
    a_send,
    a_recv,
    own_sem,
    b_send,
    b_recv,
    p_send,
    p_recv,
):
    member = lax.axis_index("dp")
    owner = lax.axis_index("cls")
    chunks, unit, width = out_ref.shape[1:]
    capacity = chunks * owners * unit
    group = min(chunks, max(1, 256 // (owners * unit)))
    span = group * owners * unit
    half = members // 2
    place = ring_place(member)
    side = owner % 2
    step = 1 - 2 * side
    contract = (((1,), (1,)), ((), ()))

    barrier = pltpu.get_barrier_semaphore()
    for hop in range(1, owners):
        pl.semaphore_signal(
            barrier, inc=1, device_id=(member, (owner + hop) % owners), device_id_type=MESH
        )
    for hop in range(1, members):
        pl.semaphore_signal(
            barrier,
            inc=1,
            device_id=(ring_member((place + hop) % members), owner),
            device_id_type=MESH,
        )
    pl.semaphore_wait(barrier, owners + members - 2)

    mine = pl.ds(pl.multiple_of(owner * unit, unit), unit)

    def dispatch(chunk, hop):
        target = (owner + hop) % owners
        return pltpu.make_async_remote_copy(
            src_ref=out_ref.at[target, chunk],
            dst_ref=rows_ref.at[0, chunk, mine],
            send_sem=a_send.at[chunk, hop - 1],
            recv_sem=a_recv.at[chunk, hop - 1],
            device_id=(member, target),
            device_id_type=MESH,
        )

    def own_copy(chunk):
        return pltpu.make_async_copy(
            out_ref.at[owner, chunk], rows_ref.at[0, chunk, mine], own_sem.at[chunk]
        )

    def share(chunk, hop):
        target = ring_member((place + step * hop + members) % members)
        return pltpu.make_async_remote_copy(
            src_ref=rows_ref.at[0, chunk],
            dst_ref=rows_ref.at[hop, chunk],
            send_sem=b_send.at[chunk, hop - 1],
            recv_sem=b_recv.at[chunk, hop - 1],
            device_id=(target, owner),
            device_id_type=MESH,
        )

    def share_picks(hop):
        return pltpu.make_async_remote_copy(
            src_ref=picks_ref.at[0],
            dst_ref=picks_ref.at[hop],
            send_sem=p_send.at[hop - 1],
            recv_sem=p_recv.at[hop - 1],
            device_id=(ring_member((place + hop) % members), owner),
            device_id_type=MESH,
        )

    def own_rows():
        return rows_ref[0].reshape(capacity, width)

    def multiply(slot, first):
        block = rows_ref[slot, first : first + group].reshape(span, width)
        low = slot * capacity + first * owners * unit
        inner_ref[:, low : low + span] = lax.dot_general(
            own_rows(), block, contract, preferred_element_type=jnp.float32
        )
        wide = block.astype(jnp.float32)
        norms_ref[low : low + span, :] = jnp.sum(wide * wide, axis=1, keepdims=True)

    sends_half = (place // half + side) % 2 == 0
    gets_half = (place // half + side) % 2 == 1

    for chunk in range(chunks):
        own_copy(chunk).start()
        for hop in range(1, owners):
            dispatch(chunk, hop).start()
    for chunk in range(chunks):
        own_copy(chunk).wait()
        for hop in range(1, owners):
            dispatch(chunk, hop).wait_recv()

        @pl.when(sends_half)
        def _(chunk=chunk):
            share(chunk, half).start()

        for hop in range(1, half):
            share(chunk, hop).start()

    picks_ref[0] = lax.dot_general(
        table_ref[...],
        own_rows(),
        (((1,), (0,)), ((), ())),
        preferred_element_type=jnp.float32,
    ).astype(picks_ref.dtype)
    for first in range(0, chunks, group):
        multiply(0, first)
    for hop in range(1, members):
        share_picks(hop).start()

    for first in range(0, chunks, group):
        for hop in range(1, half):
            for chunk in range(first, first + group):
                share(chunk, hop).wait_recv()
            multiply(hop, first)

        @pl.when(gets_half)
        def _(first=first):
            for chunk in range(first, first + group):
                share(chunk, half).wait_recv()
            multiply(half, first)

    for hop in range(1, members):
        share_picks(hop).wait_recv()
    picks = picks_ref[0].astype(jnp.float32)
    for hop in range(1, members):
        picks = picks + picks_ref[hop].astype(jnp.float32)
    pick_norms_ref[...] = jnp.sum(picks * picks, axis=1, keepdims=True)
    picks = picks.astype(picks_ref.dtype)

    def multiply_picks(slot):
        pick_inner_ref[:, slot * capacity : (slot + 1) * capacity] = lax.dot_general(
            picks,
            rows_ref[slot].reshape(capacity, width),
            contract,
            preferred_element_type=jnp.float32,
        )

    for slot in range(half):
        multiply_picks(slot)

    @pl.when(gets_half)
    def _():
        multiply_picks(half)

    for chunk in range(chunks):
        for hop in range(1, owners):
            dispatch(chunk, hop).wait_send()
        for hop in range(1, half):
            share(chunk, hop).wait_send()

        @pl.when(sends_half)
        def _(chunk=chunk):
            share(chunk, half).wait_send()

    for hop in range(1, members):
        share_picks(hop).wait_send()


def exchange(outgoing, pick_table, members, owners):
    chunks, unit, width = outgoing.shape[1:]
    capacity = chunks * owners * unit
    padded = pick_table.shape[0]
    slots = members // 2 + 1
    vmem = pl.BlockSpec(memory_space=pltpu.VMEM)
    return pl.pallas_call(
        functools.partial(exchange_kernel, members, owners),
        out_shape=(
            jax.ShapeDtypeStruct((capacity, slots * capacity), jnp.float32),
            jax.ShapeDtypeStruct((padded, slots * capacity), jnp.float32),
            jax.ShapeDtypeStruct((slots * capacity, 1), jnp.float32),
            jax.ShapeDtypeStruct((padded, 1), jnp.float32),
        ),
        in_specs=[vmem, vmem],
        out_specs=(vmem, vmem, vmem, vmem),
        scratch_shapes=[
            pltpu.VMEM((slots, chunks, owners * unit, width), outgoing.dtype),
            pltpu.VMEM((members, padded, width), outgoing.dtype),
            pltpu.SemaphoreType.DMA((chunks, owners - 1)),
            pltpu.SemaphoreType.DMA((chunks, owners - 1)),
            pltpu.SemaphoreType.DMA((chunks,)),
            pltpu.SemaphoreType.DMA((chunks, members // 2)),
            pltpu.SemaphoreType.DMA((chunks, members // 2)),
            pltpu.SemaphoreType.DMA((members - 1,)),
            pltpu.SemaphoreType.DMA((members - 1,)),
        ],
        compiler_params=pltpu.CompilerParams(
            collective_id=0, has_side_effects=True, vmem_limit_bytes=60 * 1024 * 1024
        ),
    )(outgoing, pick_table)


def body(sketches, labels, places, counts, chosen):
    row_count, width = sketches.shape
    members = lax.axis_size("dp")
    owners = lax.axis_size("cls")
    devices = members * owners
    sub = 2 * row_count // devices
    capacity = devices * sub
    unit = 16
    chunks = members * sub // unit
    half = members // 2
    slots = half + 1
    member = lax.axis_index("dp")
    owner = lax.axis_index("cls")
    picked = chosen[:, 0]
    pick_count = picked.shape[0]

    target = (labels * members + places // capacity) * sub + places % sub
    send_table = (
        lax.broadcasted_iota(jnp.int32, (2 * row_count, row_count), 0) == target[None, :]
    ).astype(jnp.bfloat16)
    outgoing = jnp.dot(send_table, sketches, preferred_element_type=jnp.float32).astype(
        jnp.bfloat16
    )
    step = 1 - 2 * (owner % 2)
    place = ring_place(member)
    slot_member = jnp.stack(
        [ring_member((place - step * hop + members) % members) for hop in range(slots)]
    )
    has_half = (place // half + owner % 2) % 2 == 1
    slot_here = (jnp.arange(slots) < half) | has_half

    class_counts = counts[0]
    valid_places = (
        lax.broadcasted_iota(jnp.int32, (members, devices, sub), 2) < class_counts[:, :, None]
    )
    valid_blocks = jnp.transpose(
        jnp.transpose(valid_places.reshape(members, members, owners, sub), (1, 2, 0, 3)).reshape(
            members, owners, chunks, unit
        ),
        (0, 2, 1, 3),
    ).reshape(members, capacity)
    slot_valid = (
        jnp.stack([lax.dynamic_index_in_dim(valid_blocks, slot_member[s], 0, False) for s in range(slots)])
        & slot_here[:, None]
    )
    column_valid = slot_valid.reshape(-1)
    own_valid = slot_valid[0]
    total = jnp.sum(class_counts).astype(jnp.float32)

    source = picked % capacity // sub
    offset = picked // capacity * sub + picked % sub
    pick_index = (offset // unit * owners + source % owners) * unit + offset % unit
    pick_table = (
        (jnp.arange(capacity)[None, :] == pick_index[:, None])
        & (source // owners == member)[:, None]
    ).astype(jnp.bfloat16)
    pick_table = jnp.pad(pick_table, ((0, -pick_count % 16), (0, 0)))

    inner, pick_inner, norms, pick_norms = exchange(
        outgoing.reshape(owners, chunks, unit, width), pick_table, members, owners
    )
    norms = norms[:, 0]
    spread = (norms[:capacity, None] + norms[None, :] - 2.0 * inner) / width
    pick_spread = (
        pick_norms[:pick_count] + norms[None, :] - 2.0 * pick_inner[:pick_count]
    ) / width

    largest = jnp.max(
        jnp.where(own_valid[:, None] & column_valid[None, :], spread, 0.0)
    )
    bound = jnp.max(lax.all_gather(largest.reshape(1), "dp", axis=0))

    pick_similar = bound - pick_spread
    current = jnp.zeros((slots * capacity,), jnp.float32)
    column_gain = []
    row_gain = []
    similar = bound - spread
    far = similar[:, capacity:]
    for turn in range(pick_count):
        near_cover = current[:capacity]
        column_gain.append(
            jnp.sum(
                jnp.where(
                    own_valid[:, None] & column_valid[None, :],
                    jnp.maximum(similar - near_cover[:, None], 0.0),
                    0.0,
                ),
                axis=0,
            )
        )
        row_gain.append(
            jnp.sum(
                jnp.where(
                    column_valid[None, capacity:],
                    jnp.maximum(far - current[None, capacity:], 0.0),
                    0.0,
                ),
                axis=1,
            )
        )
        current = jnp.maximum(current, pick_similar[turn])
    column_gain = jnp.stack(column_gain).reshape(pick_count, slots, capacity)
    near_gain = column_gain[:, 0] + jnp.stack(row_gain)
    own_cover = current[:capacity]

    near = jnp.concatenate([near_gain, own_cover[None]], axis=0)
    held = jnp.concatenate(
        [
            near[:, None],
            jnp.concatenate(
                [column_gain[:, 1:], jnp.zeros((1, slots - 1, capacity), jnp.float32)], axis=0
            ),
        ],
        axis=1,
    )
    spots = jnp.arange(members)[:, None] == slot_member[None, :]
    spots = spots & slot_here[None, :]
    placed = jnp.sum(jnp.where(spots[None, :, :, None], held[:, None], 0.0), axis=2)
    placed = jnp.transpose(
        placed.reshape(pick_count + 1, members, chunks, owners, unit), (0, 1, 3, 2, 4)
    ).reshape(pick_count + 1, members, owners, members, sub)
    placed = jnp.transpose(placed, (3, 0, 1, 2, 4)).reshape(members, pick_count + 1, capacity)
    summed = jnp.sum(
        lax.all_to_all(placed, "dp", split_axis=0, concat_axis=0, tiled=True), axis=0
    )
    place_valid = lax.dynamic_index_in_dim(
        valid_places.reshape(members, capacity), member, 0, keepdims=False
    ).astype(jnp.float32)
    gain_scores = (summed[:pick_count] * place_valid[None, :] / total)[:, None, :]
    coverage = (summed[pick_count] * place_valid)[None, :]
    return (gain_scores, coverage)


def solution(mesh):
    placed = (
        P(("dp", "cls"), None),
        P(("dp", "cls")),
        P(("dp", "cls")),
        P("cls", None, None),
        P(None, "cls"),
    )
    return jax.shard_map(
        body,
        mesh=mesh,
        in_specs=placed,
        out_specs=(P(None, "cls", "dp"), P("cls", "dp")),
        check_vma=False,
    )
```

```python
import functools

import jax
import jax.numpy as jnp
from jax import lax
from jax.experimental import pallas as pl
from jax.experimental.pallas import tpu as pltpu
from jax.sharding import PartitionSpec as P

MESH = pl.DeviceIdType.MESH


def ring_place(index):
    high = index // 2
    return 2 * high + (index % 2 + high) % 2


def ring_member(place):
    high = place // 2
    return 2 * high + (place % 2 + high) % 2


def exchange_kernel(
    members,
    owners,
    out_ref,
    table_ref,
    inner_ref,
    pick_inner_ref,
    norms_ref,
    pick_norms_ref,
    rows_ref,
    picks_ref,
    a_send,
    a_recv,
    own_sem,
    b_send,
    b_recv,
    p_send,
    p_recv,
):
    member = lax.axis_index("dp")
    owner = lax.axis_index("cls")
    chunks, unit, width = out_ref.shape[1:]
    capacity = chunks * owners * unit
    group = min(chunks, max(1, 256 // (owners * unit)))
    span = group * owners * unit
    half = members // 2
    place = ring_place(member)
    side = owner % 2
    step = 1 - 2 * side
    contract = (((1,), (1,)), ((), ()))

    barrier = pltpu.get_barrier_semaphore()
    for hop in range(1, owners):
        pl.semaphore_signal(
            barrier, inc=1, device_id=(member, (owner + hop) % owners), device_id_type=MESH
        )
    for hop in range(1, members):
        pl.semaphore_signal(
            barrier,
            inc=1,
            device_id=(ring_member((place + hop) % members), owner),
            device_id_type=MESH,
        )
    pl.semaphore_wait(barrier, owners + members - 2)

    mine = pl.ds(pl.multiple_of(owner * unit, unit), unit)

    def dispatch(chunk, hop):
        target = (owner + hop) % owners
        return pltpu.make_async_remote_copy(
            src_ref=out_ref.at[target, chunk],
            dst_ref=rows_ref.at[0, chunk, mine],
            send_sem=a_send.at[chunk, hop - 1],
            recv_sem=a_recv.at[chunk, hop - 1],
            device_id=(member, target),
            device_id_type=MESH,
        )

    def own_copy(chunk):
        return pltpu.make_async_copy(
            out_ref.at[owner, chunk], rows_ref.at[0, chunk, mine], own_sem.at[chunk]
        )

    def share(chunk, hop):
        target = ring_member((place + step * hop + members) % members)
        return pltpu.make_async_remote_copy(
            src_ref=rows_ref.at[0, chunk],
            dst_ref=rows_ref.at[hop, chunk],
            send_sem=b_send.at[chunk, hop - 1],
            recv_sem=b_recv.at[chunk, hop - 1],
            device_id=(target, owner),
            device_id_type=MESH,
        )

    def share_picks(hop):
        return pltpu.make_async_remote_copy(
            src_ref=picks_ref.at[0],
            dst_ref=picks_ref.at[hop],
            send_sem=p_send.at[hop - 1],
            recv_sem=p_recv.at[hop - 1],
            device_id=(ring_member((place + hop) % members), owner),
            device_id_type=MESH,
        )

    def own_rows():
        return rows_ref[0].reshape(capacity, width)

    def multiply(slot, first):
        block = rows_ref[slot, first : first + group].reshape(span, width)
        low = slot * capacity + first * owners * unit
        inner_ref[:, low : low + span] = lax.dot_general(
            own_rows(), block, contract, preferred_element_type=jnp.float32
        )
        wide = block.astype(jnp.float32)
        norms_ref[low : low + span, :] = jnp.sum(wide * wide, axis=1, keepdims=True)

    sends_half = (place // half + side) % 2 == 0
    gets_half = (place // half + side) % 2 == 1

    for chunk in range(chunks):
        own_copy(chunk).start()
        for hop in range(1, owners):
            dispatch(chunk, hop).start()
    for chunk in range(chunks):
        own_copy(chunk).wait()
        for hop in range(1, owners):
            dispatch(chunk, hop).wait_recv()

        @pl.when(sends_half)
        def _(chunk=chunk):
            share(chunk, half).start()

        for hop in range(1, half):
            share(chunk, hop).start()

    picks_ref[0] = lax.dot_general(
        table_ref[...],
        own_rows(),
        (((1,), (0,)), ((), ())),
        preferred_element_type=jnp.float32,
    ).astype(picks_ref.dtype)
    for first in range(0, chunks, group):
        multiply(0, first)
    for hop in range(1, members):
        share_picks(hop).start()

    for first in range(0, chunks, group):
        for hop in range(1, half):
            for chunk in range(first, first + group):
                share(chunk, hop).wait_recv()
            multiply(hop, first)

        @pl.when(gets_half)
        def _(first=first):
            for chunk in range(first, first + group):
                share(chunk, half).wait_recv()
            multiply(half, first)

    for hop in range(1, members):
        share_picks(hop).wait_recv()
    picks = picks_ref[0].astype(jnp.float32)
    for hop in range(1, members):
        picks = picks + picks_ref[hop].astype(jnp.float32)
    pick_norms_ref[...] = jnp.sum(picks * picks, axis=1, keepdims=True)
    picks = picks.astype(picks_ref.dtype)

    def multiply_picks(slot):
        pick_inner_ref[:, slot * capacity : (slot + 1) * capacity] = lax.dot_general(
            picks,
            rows_ref[slot].reshape(capacity, width),
            contract,
            preferred_element_type=jnp.float32,
        )

    for slot in range(half):
        multiply_picks(slot)

    @pl.when(gets_half)
    def _():
        multiply_picks(half)

    for chunk in range(chunks):
        for hop in range(1, owners):
            dispatch(chunk, hop).wait_send()
        for hop in range(1, half):
            share(chunk, hop).wait_send()

        @pl.when(sends_half)
        def _(chunk=chunk):
            share(chunk, half).wait_send()

    for hop in range(1, members):
        share_picks(hop).wait_send()


def exchange(outgoing, pick_table, members, owners):
    chunks, unit, width = outgoing.shape[1:]
    capacity = chunks * owners * unit
    padded = pick_table.shape[0]
    slots = members // 2 + 1
    vmem = pl.BlockSpec(memory_space=pltpu.VMEM)
    return pl.pallas_call(
        functools.partial(exchange_kernel, members, owners),
        out_shape=(
            jax.ShapeDtypeStruct((capacity, slots * capacity), jnp.float32),
            jax.ShapeDtypeStruct((padded, slots * capacity), jnp.float32),
            jax.ShapeDtypeStruct((slots * capacity, 1), jnp.float32),
            jax.ShapeDtypeStruct((padded, 1), jnp.float32),
        ),
        in_specs=[vmem, vmem],
        out_specs=(vmem, vmem, vmem, vmem),
        scratch_shapes=[
            pltpu.VMEM((slots, chunks, owners * unit, width), outgoing.dtype),
            pltpu.VMEM((members, padded, width), outgoing.dtype),
            pltpu.SemaphoreType.DMA((chunks, owners - 1)),
            pltpu.SemaphoreType.DMA((chunks, owners - 1)),
            pltpu.SemaphoreType.DMA((chunks,)),
            pltpu.SemaphoreType.DMA((chunks, members // 2)),
            pltpu.SemaphoreType.DMA((chunks, members // 2)),
            pltpu.SemaphoreType.DMA((members - 1,)),
            pltpu.SemaphoreType.DMA((members - 1,)),
        ],
        compiler_params=pltpu.CompilerParams(
            collective_id=0, has_side_effects=True, vmem_limit_bytes=60 * 1024 * 1024
        ),
    )(outgoing, pick_table)


def body(sketches, labels, places, counts, chosen):
    row_count, width = sketches.shape
    members = lax.axis_size("dp")
    owners = lax.axis_size("cls")
    devices = members * owners
    sub = 2 * row_count // devices
    capacity = devices * sub
    unit = 16
    chunks = members * sub // unit
    half = members // 2
    slots = half + 1
    member = lax.axis_index("dp")
    owner = lax.axis_index("cls")
    picked = chosen[:, 0]
    pick_count = picked.shape[0]

    target = (labels * members + places // capacity) * sub + places % sub
    send_table = (
        lax.broadcasted_iota(jnp.int32, (2 * row_count, row_count), 0) == target[None, :]
    ).astype(jnp.bfloat16)
    outgoing = jnp.dot(send_table, sketches, preferred_element_type=jnp.float32).astype(
        jnp.bfloat16
    )
    step = 1 - 2 * (owner % 2)
    place = ring_place(member)
    slot_member = jnp.stack(
        [ring_member((place - step * hop + members) % members) for hop in range(slots)]
    )
    has_half = (place // half + owner % 2) % 2 == 1
    slot_here = (jnp.arange(slots) < half) | has_half

    class_counts = counts[0]
    valid_places = (
        lax.broadcasted_iota(jnp.int32, (members, devices, sub), 2) < class_counts[:, :, None]
    )
    valid_blocks = jnp.transpose(
        jnp.transpose(valid_places.reshape(members, members, owners, sub), (1, 2, 0, 3)).reshape(
            members, owners, chunks, unit
        ),
        (0, 2, 1, 3),
    ).reshape(members, capacity)
    slot_valid = (
        jnp.stack([lax.dynamic_index_in_dim(valid_blocks, slot_member[s], 0, False) for s in range(slots)])
        & slot_here[:, None]
    )
    column_valid = slot_valid.reshape(-1)
    own_valid = slot_valid[0]
    total = jnp.sum(class_counts).astype(jnp.float32)

    source = picked % capacity // sub
    offset = picked // capacity * sub + picked % sub
    pick_index = (offset // unit * owners + source % owners) * unit + offset % unit
    pick_table = (
        (jnp.arange(capacity)[None, :] == pick_index[:, None])
        & (source // owners == member)[:, None]
    ).astype(jnp.bfloat16)
    pick_table = jnp.pad(pick_table, ((0, -pick_count % 16), (0, 0)))

    inner, pick_inner, norms, pick_norms = exchange(
        outgoing.reshape(owners, chunks, unit, width), pick_table, members, owners
    )
    norms = norms[:, 0]
    spread = (norms[:capacity, None] + norms[None, :] - 2.0 * inner) / width
    pick_spread = (
        pick_norms[:pick_count] + norms[None, :] - 2.0 * pick_inner[:pick_count]
    ) / width

    largest = jnp.max(
        jnp.where(own_valid[:, None] & column_valid[None, :], spread, 0.0)
    )
    bound = jnp.max(
        lax.all_to_all(
            jnp.broadcast_to(largest, (members, 1, 128)), "dp", split_axis=0, concat_axis=0, tiled=True
        )
    )

    pick_similar = bound - pick_spread
    current = jnp.zeros((slots * capacity,), jnp.float32)
    column_gain = []
    row_gain = []
    similar = bound - spread
    far = similar[:, capacity:]
    for turn in range(pick_count):
        near_cover = current[:capacity]
        column_gain.append(
            jnp.sum(
                jnp.where(
                    own_valid[:, None] & column_valid[None, :],
                    jnp.maximum(similar - near_cover[:, None], 0.0),
                    0.0,
                ),
                axis=0,
            )
        )
        row_gain.append(
            jnp.sum(
                jnp.where(
                    column_valid[None, capacity:],
                    jnp.maximum(far - current[None, capacity:], 0.0),
                    0.0,
                ),
                axis=1,
            )
        )
        current = jnp.maximum(current, pick_similar[turn])
    column_gain = jnp.stack(column_gain).reshape(pick_count, slots, capacity)
    near_gain = column_gain[:, 0] + jnp.stack(row_gain)
    own_cover = current[:capacity]

    near = jnp.concatenate([near_gain, own_cover[None]], axis=0)
    held = jnp.concatenate(
        [
            near[:, None],
            jnp.concatenate(
                [column_gain[:, 1:], jnp.zeros((1, slots - 1, capacity), jnp.float32)], axis=0
            ),
        ],
        axis=1,
    )
    spots = jnp.arange(members)[:, None] == slot_member[None, :]
    spots = spots & slot_here[None, :]
    placed = jnp.sum(jnp.where(spots[None, :, :, None], held[:, None], 0.0), axis=2)
    placed = jnp.transpose(
        placed.reshape(pick_count + 1, members, chunks, owners, unit), (0, 1, 3, 2, 4)
    ).reshape(pick_count + 1, members, owners, members, sub)
    placed = jnp.transpose(placed, (3, 0, 1, 2, 4)).reshape(members, pick_count + 1, capacity)
    summed = jnp.sum(
        lax.all_to_all(placed, "dp", split_axis=0, concat_axis=0, tiled=True), axis=0
    )
    place_valid = lax.dynamic_index_in_dim(
        valid_places.reshape(members, capacity), member, 0, keepdims=False
    ).astype(jnp.float32)
    gain_scores = (summed[:pick_count] * place_valid[None, :] / total)[:, None, :]
    coverage = (summed[pick_count] * place_valid)[None, :]
    return (gain_scores, coverage)


def solution(mesh):
    placed = (
        P(("dp", "cls"), None),
        P(("dp", "cls")),
        P(("dp", "cls")),
        P("cls", None, None),
        P(None, "cls"),
    )
    return jax.shard_map(
        body,
        mesh=mesh,
        in_specs=placed,
        out_specs=(P(None, "cls", "dp"), P("cls", "dp")),
        check_vma=False,
    )
```
